32 devices in a mesh: seq: 8 (over z, x), tp: 4 (over y, core).
Axes of the slice: x: 2, y: 2, z: 4, core: 2. Of those that a mesh axis runs over, the one named last changes fastest.
Arguments:
- query_rows: bfloat16 [1536, 4096], P('seq', 'tp'), may hold values from -120 to 120
- key_rows: bfloat16 [1536, 1024], P('seq', 'tp'), may hold values from -6 to 6
- value_rows: bfloat16 [1536, 1024], P('seq', 'tp'), may hold values from -6 to 6
- document_ids: int32 [1536], replicated, may hold values from 0 to 3, never falling along the last dimension, each value on 1 to 768 neighbouring positions
- output_weight: bfloat16 [4096, 8192], P('tp'), may hold values from -0.09375 to 0.09375
Outputs:
- attended: bfloat16 [1536, 8192], P(('seq', 'tp'))
The draws below stay inside these ranges and needn't reach their ends.
Inputs may be any that keep to these rules, and one draw needn't show every extreme that they name: `document_ids`: never falling along the sequence; every document holds at most 768 tokens, and one holds exactly 768.
All inputs are finite; a program needn't handle non-finite values.
Results may differ from the reference program's by a relative error of at most 0.014.
Values may be sent and summed in bfloat16 or wider, within the bound.
A program may use at most 64 MiB of HBM per device.

```python
import math
import jax
import jax.numpy as jnp
import numpy as np
from jax import lax

D = 8192
HEADS = 32
KV = 8
HD = 128
TOK_DEV = 192
SEQ = 1536
MAXDOC = 768
N_TP = 4


def query_key_pair(key):
    key_query, key_keys = jax.random.split(key, 2)
    keys_drawn = jnp.clip(jax.random.normal(key_keys, (SEQ, KV * HD), jnp.float32), -6.0, 6.0)
    queries = jnp.clip(jax.random.normal(key_query, (SEQ, HEADS * HD), jnp.float32), -6.0, 6.0)
    return (queries, keys_drawn)


def draw_query_rows(key, part):
    return query_key_pair(jax.random.fold_in(key, 11))[0].astype(jnp.bfloat16)


def draw_key_rows(key, part):
    return query_key_pair(jax.random.fold_in(key, 11))[1].astype(jnp.bfloat16)


def level_of(own_key, dims, cuts, least, top_value):
    def one(dim, shards_of):
        draws = jax.random.uniform(jax.random.fold_in(jax.random.fold_in(own_key, 6), dim), (shards_of,), jnp.float32, least / len(cuts), top_value / len(cuts))
        return jnp.repeat(jnp.exp(draws), dims[dim] // shards_of).reshape((-1,) + (1,) * (len(dims) - dim - 1))

    loudness = one(*cuts[0])
    for cut in cuts[1:]:
        loudness = loudness * one(*cut)
    return loudness


def length_profile(amount, total, most, slope):
    loads = [(1 << 20) // math.isqrt(grade ** slope) + 1 for grade in range(2, amount + 1)]
    rest, counts = total - most - (amount - 1), [1] * (amount - 1)
    while rest > 0:
        free = [i for i in range(amount - 1) if counts[i] < most]
        whole, remaining = sum([loads[i] for i in free]), rest
        for i in free:
            addition = min(most - counts[i], max(1, remaining * loads[i] // whole), rest)
            counts[i] = counts[i] + addition
            rest = rest - addition
    return np.array([most] + counts)


def ragged(key, amount, total, most, skew):
    if amount == 2:
        one = jax.random.randint(key, (), max(1, total - most), min(most, total - 1) + 1)
        return jnp.stack([one, total - one])
    sizes = jnp.asarray(length_profile(amount, total, most, skew), jnp.int32)
    twos = (amount - 1) // 2
    donor, receiver = sizes[1:1 + 2 * twos:2], sizes[2:2 + 2 * twos:2]
    room = jnp.minimum(donor - 1, most - receiver)
    shifted = jax.random.randint(jax.random.fold_in(key, 1), (twos,), 0, 1 << 20) % (room + 1)
    sizes = sizes.at[1:1 + 2 * twos:2].set(donor - shifted).at[2:2 + 2 * twos:2].set(receiver + shifted)
    return sizes[jax.random.permutation(jax.random.fold_in(key, 2), amount)]


def bell_draw(key, shape, scale, bound, shards=(), kind=jnp.bfloat16):
    gain = level_of(key, shape, shards, -0.22, 0.18) if shards else 1.0
    entries = jax.random.normal(key, shape, jnp.float32) * scale * gain
    return jnp.minimum(jnp.maximum(entries, -bound), bound).astype(kind)


def setup_inputs(seed: int = 0) -> dict:
    keys = jax.random.split(jax.random.key(seed), 6)
    query_rows = draw_query_rows(jax.random.fold_in(keys[5], 71), 0)
    key_rows = draw_key_rows(jax.random.fold_in(keys[5], 71), 0)
    value_rows = bell_draw(keys[2], (SEQ, KV * HD), 1.0, 6.0, ((0, 8), (1, 4)))
    document_ids = jnp.searchsorted(jnp.cumsum(ragged(keys[3], 2 * SEQ // MAXDOC, SEQ, MAXDOC, 2)), jnp.arange(SEQ), side="right").astype(jnp.int32)
    output_weight = bell_draw(keys[4], (HEADS * HD, D), (HEADS * HD) ** -0.5, 0.09375, ((0, 4),))
    return dict(query_rows=query_rows, key_rows=key_rows, value_rows=value_rows, document_ids=document_ids, output_weight=output_weight)


def reference(query_rows, key_rows, value_rows, document_ids, output_weight):
    group = HEADS // KV
    query_block = 4 * TOK_DEV
    key_span = min(SEQ, MAXDOC + query_block)
    block_count = SEQ // query_block
    scaling = 1.0 / (HD ** 0.5)

    def one_block(block_index):
        query_start = (block_index * query_block).astype(jnp.int32)
        key_start = jnp.clip(query_start + query_block - key_span, 0, SEQ - key_span).astype(jnp.int32)
        queries = lax.dynamic_slice_in_dim(query_rows, query_start, query_block, 0)
        queries = queries.reshape(query_block, KV, group, HD).astype(jnp.float32)
        key_block = lax.dynamic_slice_in_dim(key_rows, key_start, key_span, 0)
        key_block = key_block.reshape(key_span, KV, HD).astype(jnp.float32)
        value_block = lax.dynamic_slice_in_dim(value_rows, key_start, key_span, 0)
        value_block = value_block.reshape(key_span, KV, HD).astype(jnp.float32)
        query_doc = lax.dynamic_slice_in_dim(document_ids, query_start, query_block, 0)
        key_doc = lax.dynamic_slice_in_dim(document_ids, key_start, key_span, 0)
        query_pos = query_start + jnp.arange(query_block, dtype=jnp.int32)
        key_pos = key_start + jnp.arange(key_span, dtype=jnp.int32)
        allowed = (key_doc[None, :] == query_doc[:, None]) & (key_pos[None, :] <= query_pos[:, None])
        scores = jnp.einsum("tkgd,ukd->kgtu", queries, key_block) * scaling
        scores = jnp.where(allowed, scores, -jnp.inf)
        row_max = jnp.max(scores, axis=-1, keepdims=True)
        exponent = jnp.exp(scores - row_max)
        denominator = jnp.sum(exponent, axis=-1)
        rounded = lax.optimization_barrier(exponent.astype(jnp.bfloat16))
        context = jnp.einsum("kgtu,ukd->kgtd", rounded.astype(jnp.float32), value_block)
        context = context / denominator[..., None]
        return context.transpose(2, 0, 1, 3).reshape(query_block, HEADS * HD)

    context = lax.map(one_block, jnp.arange(block_count, dtype=jnp.int32))
    context = context.reshape(SEQ, HEADS * HD).astype(jnp.bfloat16)
    width = HEADS * HD // N_TP
    summed = jnp.zeros((SEQ, D), jnp.float32)
    for group_index in range(N_TP):
        partial_value = jnp.dot(context[:, group_index * width:(group_index + 1) * width],
                          output_weight[group_index * width:(group_index + 1) * width],
                          preferred_element_type=jnp.float32)
        partial_value = lax.optimization_barrier(partial_value.astype(jnp.bfloat16))
        summed = summed + partial_value.astype(jnp.float32)
    return summed.astype(jnp.bfloat16)
```

```python
import functools

import jax
import jax.numpy as jnp
from jax import lax
from jax.experimental import pallas as pl
from jax.experimental.pallas import tpu as pltpu
from jax.sharding import PartitionSpec as P

HEADS = 32
KV = 8
HD = 128
GROUP = HEADS // KV
MESH = pl.DeviceIdType.MESH
LOG2E = 1.4426950408889634
SCALE = LOG2E / HD**0.5
MASKED = -1e30
CHUNKS = 16


def kernel(
    n_seq, n_tp, reach,
    q_hbm, k_hbm, v_hbm, doc_ref, w_hbm, out_ref,
    q_all, q, kv, w, m, l, acc, ctx, res, d2d_src, d2d_dst, y_src, y_dst, fin,
    q_sem, own_sem, w_sem, recv_sem, zsend_sem, xsend_sem,
    d2d_send, d2d_recv, y_send, y_recv,
):
    s = lax.axis_index("seq")
    t = lax.axis_index("tp")
    tokens = q_hbm.shape[0]
    heads_kv = k_hbm.shape[1] // HD
    pieces = 2 * heads_kv
    chips = n_tp // 2
    rows = tokens // n_tp
    width = out_ref.shape[1] // CHUNKS
    odd = s % 2
    partner = s + 1 - 2 * odd
    core = t % 2
    chip = t // 2
    sibling = t + 1 - 2 * core

    def q_copy():
        return pltpu.make_async_copy(q_hbm, q_all, q_sem)

    def own_copy(c):
        src = k_hbm if c % 2 == 0 else v_hbm
        return pltpu.make_async_copy(
            src.at[:, pl.ds((c // 2) * HD, HD)], kv.at[0, c], own_sem.at[c]
        )

    def w_copy(j):
        cols = pl.ds(pl.multiple_of(j * width, width), width)
        return pltpu.make_async_copy(w_hbm.at[:, cols], w.at[:, cols], w_sem.at[j])

    for c in range(pieces):
        own_copy(c).start()
    q_copy().start()

    barrier = pltpu.get_barrier_semaphore()

    def greet(seq_index, tp_index):
        pl.semaphore_signal(
            barrier, inc=1, device_id=(seq_index, tp_index), device_id_type=MESH
        )

    greet(partner, t)
    greet(s, sibling)
    for step in range(1, chips):
        greet(s, ((chip + step) % chips) * 2 + core)

    @pl.when(s >= 2)
    def _():
        greet(s - 2, t)

    @pl.when(s + 2 < n_seq)
    def _():
        greet(s + 2, t)

    for j in range(CHUNKS):
        w_copy(j).start()

    along = (s >= 2).astype(jnp.int32) + (s + 2 < n_seq).astype(jnp.int32)
    pl.semaphore_wait(barrier, chips + 1 + along)

    def z_copy(d, c):
        return pltpu.make_async_remote_copy(
            src_ref=kv.at[d, c], dst_ref=kv.at[d + 2, c],
            send_sem=zsend_sem.at[d, c], recv_sem=recv_sem.at[d + 2, c],
            device_id=(s + 2, t), device_id_type=MESH,
        )

    def x_copy(d, to, c):
        return pltpu.make_async_remote_copy(
            src_ref=kv.at[d, c], dst_ref=kv.at[to, c],
            send_sem=xsend_sem.at[d, c], recv_sem=recv_sem.at[to, c],
            device_id=(partner, t), device_id_type=MESH,
        )

    def arrival(d, c):
        return pltpu.make_async_remote_copy(
            src_ref=kv.at[d, c], dst_ref=kv.at[d, c],
            send_sem=xsend_sem.at[d, c], recv_sem=recv_sem.at[d, c],
            device_id=(partner, t), device_id_type=MESH,
        )

    def for_sends(d, act):
        if d + 2 <= reach:
            @pl.when((s >= d) & (s + 2 < n_seq))
            def _():
                act(lambda c: z_copy(d, c))
        if d + 1 <= reach:
            @pl.when((s >= d) & (odd == 0))
            def _():
                act(lambda c: x_copy(d, d + 1, c))
        if d >= 2:
            @pl.when((s >= d) & (odd == 1))
            def _():
                act(lambda c: x_copy(d, d - 1, c))

    for c in range(pieces):
        own_copy(c).wait()
        for_sends(0, lambda copy, c=c: copy(c).start())

    q_copy().wait()
    for h in range(heads_kv * GROUP):
        q[h // GROUP, pl.ds((h % GROUP) * tokens, tokens), :] = q_all[:, h * HD:(h + 1) * HD]

    row_of = lax.broadcasted_iota(jnp.int32, (tokens, tokens), 0)
    col_of = lax.broadcasted_iota(jnp.int32, (tokens, tokens), 1)
    own_doc = doc_ref[pl.ds(s, 1), :].astype(jnp.float32)
    doc_col = jnp.sum(jnp.where(row_of == col_of, own_doc, 0.0), axis=1, keepdims=True)

    def attend(d, g):
        key_doc = doc_ref[pl.ds(s - d, 1), :].astype(jnp.float32)
        allowed = key_doc == doc_col
        if d == 0:
            allowed = allowed & (col_of <= row_of)
        bias = jnp.where(allowed, 0.0, MASKED)
        scores = lax.dot_general(
            q[g], kv[d, 2 * g], (((1,), (1,)), ((), ())), preferred_element_type=jnp.float32
        )
        scores = scores.reshape(GROUP, tokens, tokens) * SCALE + bias[None]
        scores = scores.reshape(GROUP * tokens, tokens)
        top = jnp.max(scores, axis=1, keepdims=True)
        if d == 0:
            new_m = top
        else:
            old_m = m[g]
            new_m = jnp.maximum(old_m, top)
        p = jnp.exp2(scores - new_m)
        total = jnp.sum(p, axis=1, keepdims=True)
        if d > 0:
            arrival(d, 2 * g + 1).wait_recv()
            if d % 2 == 0:
                for_sends(d, lambda copy: copy(2 * g + 1).start())
        added = jnp.dot(
            p.astype(jnp.bfloat16), kv[d, 2 * g + 1], preferred_element_type=jnp.float32
        )
        m[g] = new_m
        if d == 0:
            l[g] = total
            acc[g] = added
        else:
            rescale = jnp.exp2(old_m - new_m)
            l[g] = l[g] * rescale + total
            acc[g] = acc[g] * rescale + added

    order = [0]
    for d in range(2, reach + 1, 2):
        order += [d, d - 1]
    for d in order:
        @pl.when(s >= d)
        def _(d=d):
            @pl.loop(0, heads_kv)
            def _(g):
                if d > 0:
                    arrival(d, 2 * g).wait_recv()
                    if d % 2 == 0:
                        for_sends(d, lambda copy: copy(2 * g).start())
                attend(d, g)

    for h in range(heads_kv * GROUP):
        g, part = h // GROUP, pl.ds((h % GROUP) * tokens, tokens)
        ctx[:, h * HD:(h + 1) * HD] = (acc[g, part, :] / l[g, part, :]).astype(jnp.bfloat16)

    def d2d_copy(j):
        return pltpu.make_async_remote_copy(
            src_ref=d2d_src.at[j], dst_ref=d2d_dst.at[j],
            send_sem=d2d_send.at[j], recv_sem=d2d_recv.at[j],
            device_id=(s, sibling), device_id_type=MESH,
        )

    def y_copy(j, step):
        return pltpu.make_async_remote_copy(
            src_ref=y_src.at[j, step - 1], dst_ref=y_dst.at[j, step - 1],
            send_sem=y_send.at[j, step - 1], recv_sem=y_recv.at[j, step - 1],
            device_id=(s, ((chip + step) % chips) * 2 + core), device_id_type=MESH,
        )

    def rows_of(j, owner):
        return res[j % 2, pl.ds(pl.multiple_of(owner * rows, 8), rows), :]

    def project(j):
        w_copy(j).wait()
        cols = pl.ds(pl.multiple_of(j * width, width), width)
        res[j % 2] = jnp.dot(ctx[...], w[:, cols], preferred_element_type=jnp.float32)
        for y in range(chips):
            d2d_src[j, y] = rows_of(j, y * 2 + 1 - core).astype(jnp.bfloat16)
        d2d_copy(j).start()

    def pair_up(j):
        d2d_copy(j).wait_recv()
        for step in range(1, chips):
            other = (chip + step) % chips
            pair = rows_of(j, other * 2 + core) + d2d_dst[j, other].astype(jnp.float32)
            y_src[j, step - 1] = pair.astype(jnp.bfloat16)
            y_copy(j, step).start()
        fin[j] = rows_of(j, t) + d2d_dst[j, chip].astype(jnp.float32)

    project(0)

    @pl.loop(1, CHUNKS)
    def _(j):
        project(j)
        pair_up(j - 1)

    pair_up(CHUNKS - 1)

    @pl.loop(0, CHUNKS)
    def _(j):
        total = fin[j]
        for step in range(1, chips):
            y_copy(j, step).wait_recv()
            total = total + y_dst[j, step - 1].astype(jnp.float32)
        cols = pl.ds(pl.multiple_of(j * width, width), width)
        out_ref[:, cols] = total.astype(out_ref.dtype)

    for d in range(0, reach + 1, 2):
        def drain(copy):
            for c in range(pieces):
                copy(c).wait_send()
        for_sends(d, drain)

    @pl.loop(0, CHUNKS)
    def _(j):
        d2d_copy(j).wait_send()
        for step in range(1, chips):
            y_copy(j, step).wait_send()


def solution(mesh):
    n_seq, n_tp = mesh.shape["seq"], mesh.shape["tp"]
    reach = min(12, n_seq // 2)
    chips = n_tp // 2

    def per_device(query_rows, key_rows, value_rows, document_ids, output_weight):
        tokens, q_width = query_rows.shape
        heads_kv = key_rows.shape[1] // HD
        depth, model = output_weight.shape
        rows, width = tokens // n_tp, model // CHUNKS
        bf16, f32 = jnp.bfloat16, jnp.float32
        dma = pltpu.SemaphoreType.DMA
        docs = document_ids.reshape(n_seq, tokens)
        any_space = pl.BlockSpec(memory_space=pl.ANY)
        in_vmem = pl.BlockSpec(memory_space=pltpu.VMEM)
        return pl.pallas_call(
            functools.partial(kernel, n_seq, n_tp, reach),
            out_shape=jax.ShapeDtypeStruct((rows, model), bf16),
            in_specs=[any_space, any_space, any_space, in_vmem, any_space],
            out_specs=in_vmem,
            scratch_shapes=[
                pltpu.VMEM((tokens, q_width), bf16),
                pltpu.VMEM((heads_kv, GROUP * tokens, HD), bf16),
                pltpu.VMEM((reach + 1, 2 * heads_kv, tokens, HD), bf16),
                pltpu.VMEM((depth, model), bf16),
                pltpu.VMEM((heads_kv, GROUP * tokens, 1), f32),
                pltpu.VMEM((heads_kv, GROUP * tokens, 1), f32),
                pltpu.VMEM((heads_kv, GROUP * tokens, HD), f32),
                pltpu.VMEM((tokens, q_width), bf16),
                pltpu.VMEM((2, tokens, width), f32),
                pltpu.VMEM((CHUNKS, chips, rows, width), bf16),
                pltpu.VMEM((CHUNKS, chips, rows, width), bf16),
                pltpu.VMEM((CHUNKS, chips - 1, rows, width), bf16),
                pltpu.VMEM((CHUNKS, chips - 1, rows, width), bf16),
                pltpu.VMEM((CHUNKS, rows, width), f32),
                dma, dma((2 * heads_kv,)), dma((CHUNKS,)),
                dma((reach + 1, 2 * heads_kv)),
                dma((reach + 1, 2 * heads_kv)),
                dma((reach + 1, 2 * heads_kv)),
                dma((CHUNKS,)), dma((CHUNKS,)),
                dma((CHUNKS, chips - 1)), dma((CHUNKS, chips - 1)),
            ],
            compiler_params=pltpu.CompilerParams(
                collective_id=0, has_side_effects=True, vmem_limit_bytes=60 * 1024 * 1024
            ),
        )(query_rows, key_rows, value_rows, docs, output_weight)

    in_specs = (P("seq", "tp"), P("seq", "tp"), P("seq", "tp"), P(), P("tp", None))
    return jax.shard_map(
        per_device, mesh=mesh, in_specs=in_specs, out_specs=P(("seq", "tp"), None),
        check_vma=False,
    )
```

```python
import functools
import math

import jax
import jax.numpy as jnp
from jax import lax
from jax.experimental import pallas as pl
from jax.experimental.pallas import tpu as pltpu
from jax.sharding import PartitionSpec as P

HEADS = 32
KV = 8
HD = 128
GROUP = HEADS // KV
MESH = pl.DeviceIdType.MESH
LOG2E = 1.4426950408889634
SCALE = LOG2E / HD**0.5
MASKED = -1e30
CHUNKS = 16


def kernel(
    n_seq, n_tp, reach,
    q_hbm, k_hbm, v_hbm, doc_hbm, w_hbm, out_ref,
    q_all, q, kv, w, docs, q_doc, q_pos, key_docs, m, l, acc, ctx, res, d2d_src, d2d_dst, y_src, y_dst, fin,
    q_sem, doc_sem, own_sem, w_sem, recv_sem, zsend_sem, xsend_sem,
    d2d_send, d2d_recv, y_send, y_recv,
):
    s = lax.axis_index("seq")
    t = lax.axis_index("tp")
    tokens = q_hbm.shape[0]
    heads_kv = k_hbm.shape[1] // HD
    pieces = 2 * heads_kv
    chips = n_tp // 2
    rows = tokens // n_tp
    width = out_ref.shape[1] // CHUNKS
    odd = s % 2
    partner = s + 1 - 2 * odd
    core = t % 2
    chip = t // 2
    sibling = t + 1 - 2 * core
    tile = math.gcd(GROUP * tokens, 256)

    def q_copy():
        return pltpu.make_async_copy(q_hbm, q_all, q_sem)

    def doc_copy():
        return pltpu.make_async_copy(doc_hbm, docs, doc_sem)

    def own_copy(c):
        src = k_hbm if c % 2 == 0 else v_hbm
        return pltpu.make_async_copy(
            src.at[:, pl.ds((c // 2) * HD, HD)], kv.at[0, c], own_sem.at[c]
        )

    def w_copy(j):
        cols = pl.ds(pl.multiple_of(j * width, width), width)
        return pltpu.make_async_copy(w_hbm.at[:, cols], w.at[:, cols], w_sem.at[j])

    for c in range(pieces):
        own_copy(c).start()
    q_copy().start()
    doc_copy().start()

    barrier = pltpu.get_barrier_semaphore()

    def greet(seq_index, tp_index):
        pl.semaphore_signal(
            barrier, inc=1, device_id=(seq_index, tp_index), device_id_type=MESH
        )

    greet(partner, t)
    greet(s, sibling)
    for step in range(1, chips):
        greet(s, ((chip + step) % chips) * 2 + core)

    @pl.when(s >= 2)
    def _():
        greet(s - 2, t)

    @pl.when(s + 2 < n_seq)
    def _():
        greet(s + 2, t)

    for j in range(CHUNKS):
        w_copy(j).start()

    along = (s >= 2).astype(jnp.int32) + (s + 2 < n_seq).astype(jnp.int32)
    pl.semaphore_wait(barrier, chips + 1 + along)

    def z_copy(d, c):
        return pltpu.make_async_remote_copy(
            src_ref=kv.at[d, c], dst_ref=kv.at[d + 2, c],
            send_sem=zsend_sem.at[d, c], recv_sem=recv_sem.at[d + 2, c],
            device_id=(s + 2, t), device_id_type=MESH,
        )

    def x_copy(d, to, c):
        return pltpu.make_async_remote_copy(
            src_ref=kv.at[d, c], dst_ref=kv.at[to, c],
            send_sem=xsend_sem.at[d, c], recv_sem=recv_sem.at[to, c],
            device_id=(partner, t), device_id_type=MESH,
        )

    def arrival(d, c):
        return pltpu.make_async_remote_copy(
            src_ref=kv.at[d, c], dst_ref=kv.at[d, c],
            send_sem=xsend_sem.at[d, c], recv_sem=recv_sem.at[d, c],
            device_id=(partner, t), device_id_type=MESH,
        )

    def for_sends(d, act):
        if d + 2 <= reach:
            @pl.when((s >= d) & (s + 2 < n_seq))
            def _():
                act(lambda c: z_copy(d, c))
        if d + 1 <= reach:
            @pl.when((s >= d) & (odd == 0))
            def _():
                act(lambda c: x_copy(d, d + 1, c))
        if d >= 2:
            @pl.when((s >= d) & (odd == 1))
            def _():
                act(lambda c: x_copy(d, d - 1, c))

    for c in range(pieces):
        own_copy(c).wait()
        for_sends(0, lambda copy, c=c: copy(c).start())

    q_copy().wait()
    for h in range(heads_kv * GROUP):
        q[h // GROUP, pl.ds((h % GROUP) * tokens, tokens), :] = q_all[:, h * HD:(h + 1) * HD]

    doc_copy().wait()
    lanes = 128
    span = (tokens + lanes - math.gcd(tokens, lanes) + lanes - 1) // lanes
    key_of = lax.broadcasted_iota(jnp.int32, (tokens, span * lanes), 0)
    lane_of = lax.broadcasted_iota(jnp.int32, (tokens, span * lanes), 1)

    def docs_down(block):
        first = block * tokens
        top_row, shift = first // lanes, first % lanes
        ids = jnp.concatenate(
            [
                docs[pl.ds(jnp.minimum(top_row + i, docs.shape[0] - 1), 1), :]
                for i in range(span)
            ],
            axis=1,
        ).astype(jnp.float32)
        return jnp.sum(jnp.where(lane_of == key_of + shift, ids, 0.0), axis=1, keepdims=True)

    row_of = lax.broadcasted_iota(jnp.int32, (tokens, tokens), 0)
    col_of = lax.broadcasted_iota(jnp.int32, (tokens, tokens), 1)
    own_row = jnp.sum(
        jnp.where(row_of == col_of, docs_down(s), 0.0), axis=0, keepdims=True
    )
    q_doc[...] = jnp.concatenate([own_row] * GROUP, axis=1)
    q_pos[...] = jnp.concatenate([col_of[:1]] * GROUP, axis=1)
    tiles = [pl.ds(i * tile, tile) for i in range(GROUP * tokens // tile)]

    def attend(d, g):
        key_doc = key_docs[...]
        probs = []
        for cols in tiles:
            scores = lax.dot_general(
                kv[d, 2 * g], q[g, cols, :], (((1,), (1,)), ((), ())),
                preferred_element_type=jnp.float32,
            )
            allowed = key_doc == q_doc[:, cols]
            if d == 0:
                key_pos = lax.broadcasted_iota(jnp.int32, (tokens, tile), 0)
                allowed = allowed & (key_pos <= q_pos[:, cols])
            scores = jnp.where(allowed, scores * SCALE, MASKED)
            top = jnp.max(scores, axis=0, keepdims=True)
            if d == 0:
                p = jnp.exp2(scores - top)
                l[g, :, cols] = jnp.sum(p, axis=0, keepdims=True)
                m[g, :, cols] = top
                rescale = None
            else:
                old_m = m[g, :, cols]
                new_m = jnp.maximum(old_m, top)
                p = jnp.exp2(scores - new_m)
                rescale = jnp.exp2(old_m - new_m)
                l[g, :, cols] = l[g, :, cols] * rescale + jnp.sum(p, axis=0, keepdims=True)
                m[g, :, cols] = new_m
            probs.append((p.astype(jnp.bfloat16), rescale))
        if d > 0:
            arrival(d, 2 * g + 1).wait_recv()
            if d % 2 == 0:
                for_sends(d, lambda copy: copy(2 * g + 1).start())
        for cols, (p, rescale) in zip(tiles, probs):
            added = lax.dot_general(
                kv[d, 2 * g + 1], p, (((0,), (0,)), ((), ())),
                preferred_element_type=jnp.float32,
            )
            if d == 0:
                acc[g, :, cols] = added
            else:
                acc[g, :, cols] = acc[g, :, cols] * rescale + added

    order = [0]
    for d in range(2, reach + 1, 2):
        order += [d, d - 1]
    for d in order:
        @pl.when(s >= d)
        def _(d=d):
            key_docs[...] = docs_down(s - d)

            @pl.loop(0, heads_kv)
            def _(g):
                if d > 0:
                    arrival(d, 2 * g).wait_recv()
                    if d % 2 == 0:
                        for_sends(d, lambda copy: copy(2 * g).start())
                attend(d, g)

    for g in range(heads_kv):
        mixed = jnp.transpose(acc[g] / l[g]).astype(jnp.bfloat16)
        for i in range(GROUP):
            h = g * GROUP + i
            ctx[:, h * HD:(h + 1) * HD] = mixed[i * tokens:(i + 1) * tokens, :]

    def d2d_copy(j):
        return pltpu.make_async_remote_copy(
            src_ref=d2d_src.at[j], dst_ref=d2d_dst.at[j],
            send_sem=d2d_send.at[j], recv_sem=d2d_recv.at[j],
            device_id=(s, sibling), device_id_type=MESH,
        )

    def y_copy(j, step):
        return pltpu.make_async_remote_copy(
            src_ref=y_src.at[j, step - 1], dst_ref=y_dst.at[j, step - 1],
            send_sem=y_send.at[j, step - 1], recv_sem=y_recv.at[j, step - 1],
            device_id=(s, ((chip + step) % chips) * 2 + core), device_id_type=MESH,
        )

    def rows_of(j, owner):
        return res[j % 2, pl.ds(pl.multiple_of(owner * rows, 8), rows), :]

    def project(j):
        w_copy(j).wait()
        cols = pl.ds(pl.multiple_of(j * width, width), width)
        res[j % 2] = jnp.dot(ctx[...], w[:, cols], preferred_element_type=jnp.float32)
        for y in range(chips):
            d2d_src[j, y] = rows_of(j, y * 2 + 1 - core).astype(jnp.bfloat16)
        d2d_copy(j).start()

    def pair_up(j):
        d2d_copy(j).wait_recv()
        for step in range(1, chips):
            other = (chip + step) % chips
            pair = rows_of(j, other * 2 + core) + d2d_dst[j, other].astype(jnp.float32)
            y_src[j, step - 1] = pair.astype(jnp.bfloat16)
            y_copy(j, step).start()
        fin[j] = rows_of(j, t) + d2d_dst[j, chip].astype(jnp.float32)

    project(0)

    @pl.loop(1, CHUNKS)
    def _(j):
        project(j)
        pair_up(j - 1)

    pair_up(CHUNKS - 1)

    @pl.loop(0, CHUNKS)
    def _(j):
        total = fin[j]
        for step in range(1, chips):
            y_copy(j, step).wait_recv()
            total = total + y_dst[j, step - 1].astype(jnp.float32)
        cols = pl.ds(pl.multiple_of(j * width, width), width)
        out_ref[:, cols] = total.astype(out_ref.dtype)

    for d in range(0, reach + 1, 2):
        def drain(copy):
            for c in range(pieces):
                copy(c).wait_send()
        for_sends(d, drain)

    @pl.loop(0, CHUNKS)
    def _(j):
        d2d_copy(j).wait_send()
        for step in range(1, chips):
            y_copy(j, step).wait_send()


def solution(mesh):
    n_seq, n_tp = mesh.shape["seq"], mesh.shape["tp"]
    reach = min(12, n_seq // 2)
    chips = n_tp // 2

    def per_device(query_rows, key_rows, value_rows, document_ids, output_weight):
        tokens, q_width = query_rows.shape
        heads_kv = key_rows.shape[1] // HD
        depth, model = output_weight.shape
        rows, width = tokens // n_tp, model // CHUNKS
        bf16, f32 = jnp.bfloat16, jnp.float32
        dma = pltpu.SemaphoreType.DMA
        docs = document_ids.reshape(-1, 128)
        any_space = pl.BlockSpec(memory_space=pl.ANY)
        in_vmem = pl.BlockSpec(memory_space=pltpu.VMEM)
        return pl.pallas_call(
            functools.partial(kernel, n_seq, n_tp, reach),
            out_shape=jax.ShapeDtypeStruct((rows, model), bf16),
            in_specs=[any_space, any_space, any_space, any_space, any_space],
            out_specs=in_vmem,
            scratch_shapes=[
                pltpu.VMEM((tokens, q_width), bf16),
                pltpu.VMEM((heads_kv, GROUP * tokens, HD), bf16),
                pltpu.VMEM((reach + 1, 2 * heads_kv, tokens, HD), bf16),
                pltpu.VMEM((depth, model), bf16),
                pltpu.VMEM(docs.shape, jnp.int32),
                pltpu.VMEM((1, GROUP * tokens), f32),
                pltpu.VMEM((1, GROUP * tokens), jnp.int32),
                pltpu.VMEM((tokens, 1), f32),
                pltpu.VMEM((heads_kv, 1, GROUP * tokens), f32),
                pltpu.VMEM((heads_kv, 1, GROUP * tokens), f32),
                pltpu.VMEM((heads_kv, HD, GROUP * tokens), f32),
                pltpu.VMEM((tokens, q_width), bf16),
                pltpu.VMEM((2, tokens, width), f32),
                pltpu.VMEM((CHUNKS, chips, rows, width), bf16),
                pltpu.VMEM((CHUNKS, chips, rows, width), bf16),
                pltpu.VMEM((CHUNKS, chips - 1, rows, width), bf16),
                pltpu.VMEM((CHUNKS, chips - 1, rows, width), bf16),
                pltpu.VMEM((CHUNKS, rows, width), f32),
                dma, dma, dma((2 * heads_kv,)), dma((CHUNKS,)),
                dma((reach + 1, 2 * heads_kv)),
                dma((reach + 1, 2 * heads_kv)),
                dma((reach + 1, 2 * heads_kv)),
                dma((CHUNKS,)), dma((CHUNKS,)),
                dma((CHUNKS, chips - 1)), dma((CHUNKS, chips - 1)),
            ],
            compiler_params=pltpu.CompilerParams(
                collective_id=0, has_side_effects=True, vmem_limit_bytes=60 * 1024 * 1024
            ),
        )(query_rows, key_rows, value_rows, docs, output_weight)

    in_specs = (P("seq", "tp"), P("seq", "tp"), P("seq", "tp"), P(), P("tp", None))
    return jax.shard_map(
        per_device, mesh=mesh, in_specs=in_specs, out_specs=P(("seq", "tp"), None),
        check_vma=False,
    )
```

```python
import functools
import math

import jax
import jax.numpy as jnp
from jax import lax
from jax.experimental import pallas as pl
from jax.experimental.pallas import tpu as pltpu
from jax.sharding import PartitionSpec as P

HEADS = 32
KV = 8
HD = 128
GROUP = HEADS // KV
MESH = pl.DeviceIdType.MESH
LOG2E = 1.4426950408889634
SCALE = LOG2E / HD**0.5
MASKED = -1e30
CHUNKS = 16


def kernel(
    n_seq, n_tp, reach,
    q_hbm, k_hbm, v_hbm, doc_hbm, w_hbm, out_ref,
    q_all, q, kv, w, docs, q_doc, q_pos, key_docs, m, l, acc, ctx, res, d2d_src, d2d_dst, y_src, y_dst, fin,
    q_sem, doc_sem, own_sem, w_sem, recv_sem, zsend_sem, xsend_sem,
    d2d_send, d2d_recv, y_send, y_recv,
):
    s = lax.axis_index("seq")
    t = lax.axis_index("tp")
    tokens = q_hbm.shape[0]
    heads_kv = k_hbm.shape[1] // HD
    pieces = 4 * heads_kv
    half = tokens // 2
    chips = n_tp // 2
    rows = tokens // n_tp
    width = out_ref.shape[1] // CHUNKS
    odd = s % 2
    partner = s + 1 - 2 * odd
    core = t % 2
    chip = t // 2
    sibling = t + 1 - 2 * core
    tile = math.gcd(GROUP * tokens, 256)

    def q_copy():
        return pltpu.make_async_copy(q_hbm, q_all, q_sem)

    def doc_copy():
        return pltpu.make_async_copy(doc_hbm, docs, doc_sem)

    def own_copy(c):
        src = k_hbm if c % 4 < 2 else v_hbm
        return pltpu.make_async_copy(
            src.at[pl.ds((c % 2) * half, half), pl.ds((c // 4) * HD, HD)],
            kv.at[0, c], own_sem.at[c],
        )

    def w_copy(j):
        cols = pl.ds(pl.multiple_of(j * width, width), width)
        return pltpu.make_async_copy(w_hbm.at[:, cols], w.at[:, cols], w_sem.at[j])

    for c in range(pieces):
        own_copy(c).start()
    q_copy().start()
    doc_copy().start()

    barrier = pltpu.get_barrier_semaphore()

    def greet(seq_index, tp_index):
        pl.semaphore_signal(
            barrier, inc=1, device_id=(seq_index, tp_index), device_id_type=MESH
        )

    greet(partner, t)
    greet(s, sibling)
    for step in range(1, chips):
        greet(s, ((chip + step) % chips) * 2 + core)

    @pl.when(s >= 2)
    def _():
        greet(s - 2, t)

    @pl.when(s + 2 < n_seq)
    def _():
        greet(s + 2, t)

    for j in range(CHUNKS):
        w_copy(j).start()

    along = (s >= 2).astype(jnp.int32) + (s + 2 < n_seq).astype(jnp.int32)
    pl.semaphore_wait(barrier, chips + 1 + along)

    def z_copy(d, c):
        return pltpu.make_async_remote_copy(
            src_ref=kv.at[d, c], dst_ref=kv.at[d + 2, c],
            send_sem=zsend_sem.at[d, c], recv_sem=recv_sem.at[d + 2, c],
            device_id=(s + 2, t), device_id_type=MESH,
        )

    def x_copy(d, to, c):
        return pltpu.make_async_remote_copy(
            src_ref=kv.at[d, c], dst_ref=kv.at[to, c],
            send_sem=xsend_sem.at[d, c], recv_sem=recv_sem.at[to, c],
            device_id=(partner, t), device_id_type=MESH,
        )

    def arrival(d, c):
        return pltpu.make_async_remote_copy(
            src_ref=kv.at[d, c], dst_ref=kv.at[d, c],
            send_sem=xsend_sem.at[d, c], recv_sem=recv_sem.at[d, c],
            device_id=(partner, t), device_id_type=MESH,
        )

    def for_sends(d, act):
        if d + 2 <= reach:
            @pl.when((s >= d) & (s + 2 < n_seq))
            def _():
                act(lambda c: z_copy(d, c))
        if d + 1 <= reach:
            @pl.when((s >= d) & (odd == 0))
            def _():
                act(lambda c: x_copy(d, d + 1, c))
        if d >= 2:
            @pl.when((s >= d) & (odd == 1))
            def _():
                act(lambda c: x_copy(d, d - 1, c))

    def take(d, c):
        arrival(d, c).wait_recv()
        if d % 2 == 0:
            for_sends(d, lambda copy: copy(c).start())

    for c in range(pieces):
        own_copy(c).wait()
        for_sends(0, lambda copy, c=c: copy(c).start())

    q_copy().wait()
    for h in range(heads_kv * GROUP):
        q[h // GROUP, pl.ds((h % GROUP) * tokens, tokens), :] = q_all[:, h * HD:(h + 1) * HD]

    doc_copy().wait()
    lanes = 128
    span = (tokens + lanes - math.gcd(tokens, lanes) + lanes - 1) // lanes
    key_of = lax.broadcasted_iota(jnp.int32, (tokens, span * lanes), 0)
    lane_of = lax.broadcasted_iota(jnp.int32, (tokens, span * lanes), 1)

    def docs_down(block):
        first = block * tokens
        top_row, shift = first // lanes, first % lanes
        ids = jnp.concatenate(
            [
                docs[pl.ds(jnp.minimum(top_row + i, docs.shape[0] - 1), 1), :]
                for i in range(span)
            ],
            axis=1,
        ).astype(jnp.float32)
        return jnp.sum(jnp.where(lane_of == key_of + shift, ids, 0.0), axis=1, keepdims=True)

    row_of = lax.broadcasted_iota(jnp.int32, (tokens, tokens), 0)
    col_of = lax.broadcasted_iota(jnp.int32, (tokens, tokens), 1)
    own_row = jnp.sum(
        jnp.where(row_of == col_of, docs_down(s), 0.0), axis=0, keepdims=True
    )
    q_doc[...] = jnp.concatenate([own_row] * GROUP, axis=1)
    q_pos[...] = jnp.concatenate([col_of[:1]] * GROUP, axis=1)
    tiles = [pl.ds(i * tile, tile) for i in range(GROUP * tokens // tile)]

    def attend(d, g):
        key_doc = key_docs[...]
        keys = kv[d, pl.ds(4 * g, 2)].reshape(tokens, HD)
        probs = []
        for cols in tiles:
            scores = lax.dot_general(
                keys, q[g, cols, :], (((1,), (1,)), ((), ())),
                preferred_element_type=jnp.float32,
            )
            allowed = key_doc == q_doc[:, cols]
            if d == 0:
                key_pos = lax.broadcasted_iota(jnp.int32, (tokens, tile), 0)
                allowed = allowed & (key_pos <= q_pos[:, cols])
            scores = jnp.where(allowed, scores * SCALE, MASKED)
            top = jnp.max(scores, axis=0, keepdims=True)
            if d == 0:
                p = jnp.exp2(scores - top)
                l[g, :, cols] = jnp.sum(p, axis=0, keepdims=True)
                m[g, :, cols] = top
                rescale = None
            else:
                old_m = m[g, :, cols]
                new_m = jnp.maximum(old_m, top)
                p = jnp.exp2(scores - new_m)
                rescale = jnp.exp2(old_m - new_m)
                l[g, :, cols] = l[g, :, cols] * rescale + jnp.sum(p, axis=0, keepdims=True)
                m[g, :, cols] = new_m
            probs.append((p.astype(jnp.bfloat16), rescale))
        if d > 0:
            take(d, 4 * g + 2)
            take(d, 4 * g + 3)
        values = kv[d, pl.ds(4 * g + 2, 2)].reshape(tokens, HD)
        for cols, (p, rescale) in zip(tiles, probs):
            added = lax.dot_general(
                values, p, (((0,), (0,)), ((), ())),
                preferred_element_type=jnp.float32,
            )
            if d == 0:
                acc[g, :, cols] = added
            else:
                acc[g, :, cols] = acc[g, :, cols] * rescale + added

    order = [0]
    for d in range(2, reach + 1, 2):
        order += [d, d - 1]
    for d in order:
        @pl.when(s >= d)
        def _(d=d):
            key_docs[...] = docs_down(s - d)

            @pl.loop(0, heads_kv)
            def _(g):
                if d > 0:
                    take(d, 4 * g)
                    take(d, 4 * g + 1)
                attend(d, g)

    for g in range(heads_kv):
        mixed = jnp.transpose(acc[g] / l[g]).astype(jnp.bfloat16)
        for i in range(GROUP):
            h = g * GROUP + i
            ctx[:, h * HD:(h + 1) * HD] = mixed[i * tokens:(i + 1) * tokens, :]

    def d2d_copy(j):
        return pltpu.make_async_remote_copy(
            src_ref=d2d_src.at[j], dst_ref=d2d_dst.at[j],
            send_sem=d2d_send.at[j], recv_sem=d2d_recv.at[j],
            device_id=(s, sibling), device_id_type=MESH,
        )

    def y_copy(j, step):
        return pltpu.make_async_remote_copy(
            src_ref=y_src.at[j, step - 1], dst_ref=y_dst.at[j, step - 1],
            send_sem=y_send.at[j, step - 1], recv_sem=y_recv.at[j, step - 1],
            device_id=(s, ((chip + step) % chips) * 2 + core), device_id_type=MESH,
        )

    def rows_of(j, owner):
        return res[j % 2, pl.ds(pl.multiple_of(owner * rows, 8), rows), :]

    def project(j):
        w_copy(j).wait()
        cols = pl.ds(pl.multiple_of(j * width, width), width)
        res[j % 2] = jnp.dot(ctx[...], w[:, cols], preferred_element_type=jnp.float32)
        for y in range(chips):
            d2d_src[j, y] = rows_of(j, y * 2 + 1 - core).astype(jnp.bfloat16)
        d2d_copy(j).start()

    def pair_up(j):
        d2d_copy(j).wait_recv()
        for step in range(1, chips):
            other = (chip + step) % chips
            pair = rows_of(j, other * 2 + core) + d2d_dst[j, other].astype(jnp.float32)
            y_src[j, step - 1] = pair.astype(jnp.bfloat16)
            y_copy(j, step).start()
        fin[j] = rows_of(j, t) + d2d_dst[j, chip].astype(jnp.float32)

    project(0)

    @pl.loop(1, CHUNKS)
    def _(j):
        project(j)
        pair_up(j - 1)

    pair_up(CHUNKS - 1)

    @pl.loop(0, CHUNKS)
    def _(j):
        total = fin[j]
        for step in range(1, chips):
            y_copy(j, step).wait_recv()
            total = total + y_dst[j, step - 1].astype(jnp.float32)
        cols = pl.ds(pl.multiple_of(j * width, width), width)
        out_ref[:, cols] = total.astype(out_ref.dtype)

    for d in range(0, reach + 1, 2):
        def drain(copy):
            for c in range(pieces):
                copy(c).wait_send()
        for_sends(d, drain)

    @pl.loop(0, CHUNKS)
    def _(j):
        d2d_copy(j).wait_send()
        for step in range(1, chips):
            y_copy(j, step).wait_send()


def solution(mesh):
    n_seq, n_tp = mesh.shape["seq"], mesh.shape["tp"]
    reach = min(12, n_seq // 2)
    chips = n_tp // 2

    def per_device(query_rows, key_rows, value_rows, document_ids, output_weight):
        tokens, q_width = query_rows.shape
        heads_kv = key_rows.shape[1] // HD
        depth, model = output_weight.shape
        rows, width = tokens // n_tp, model // CHUNKS
        bf16, f32 = jnp.bfloat16, jnp.float32
        dma = pltpu.SemaphoreType.DMA
        docs = document_ids.reshape(-1, 128)
        in_hbm = pl.BlockSpec(memory_space=pltpu.HBM)
        in_vmem = pl.BlockSpec(memory_space=pltpu.VMEM)
        return pl.pallas_call(
            functools.partial(kernel, n_seq, n_tp, reach),
            out_shape=pltpu.VMEM((rows, model), bf16),
            in_specs=[in_hbm] * 5,
            out_specs=in_vmem,
            scratch_shapes=[
                pltpu.VMEM((tokens, q_width), bf16),
                pltpu.VMEM((heads_kv, GROUP * tokens, HD), bf16),
                pltpu.VMEM((reach + 1, 4 * heads_kv, tokens // 2, HD), bf16),
                pltpu.VMEM((depth, model), bf16),
                pltpu.VMEM(docs.shape, jnp.int32),
                pltpu.VMEM((1, GROUP * tokens), f32),
                pltpu.VMEM((1, GROUP * tokens), jnp.int32),
                pltpu.VMEM((tokens, 1), f32),
                pltpu.VMEM((heads_kv, 1, GROUP * tokens), f32),
                pltpu.VMEM((heads_kv, 1, GROUP * tokens), f32),
                pltpu.VMEM((heads_kv, HD, GROUP * tokens), f32),
                pltpu.VMEM((tokens, q_width), bf16),
                pltpu.VMEM((2, tokens, width), f32),
                pltpu.VMEM((CHUNKS, chips, rows, width), bf16),
                pltpu.VMEM((CHUNKS, chips, rows, width), bf16),
                pltpu.VMEM((CHUNKS, chips - 1, rows, width), bf16),
                pltpu.VMEM((CHUNKS, chips - 1, rows, width), bf16),
                pltpu.VMEM((CHUNKS, rows, width), f32),
                dma, dma, dma((4 * heads_kv,)), dma((CHUNKS,)),
                dma((reach + 1, 4 * heads_kv)),
                dma((reach + 1, 4 * heads_kv)),
                dma((reach + 1, 4 * heads_kv)),
                dma((CHUNKS,)), dma((CHUNKS,)),
                dma((CHUNKS, chips - 1)), dma((CHUNKS, chips - 1)),
            ],
            compiler_params=pltpu.CompilerParams(
                collective_id=0, has_side_effects=True, vmem_limit_bytes=60 * 1024 * 1024
            ),
        )(query_rows, key_rows, value_rows, docs, output_weight)

    in_specs = (P("seq", "tp"), P("seq", "tp"), P("seq", "tp"), P(), P("tp", None))
    return jax.shard_map(
        per_device, mesh=mesh, in_specs=in_specs, out_specs=P(("seq", "tp"), None),
        check_vma=False,
    )
```

```python
import functools
import math

import jax
import jax.numpy as jnp
from jax import lax
from jax.experimental import pallas as pl
from jax.experimental.pallas import tpu as pltpu
from jax.sharding import PartitionSpec as P

HEADS = 32
KV = 8
HD = 128
GROUP = HEADS // KV
MESH = pl.DeviceIdType.MESH
LOG2E = 1.4426950408889634
SCALE = LOG2E / HD**0.5
MASKED = -1e30
CHUNKS = 16


def kernel(
    n_seq, n_tp, reach,
    q_hbm, k_hbm, v_hbm, doc_hbm, w_hbm, out_ref,
    q_all, q, kv, w, docs, q_doc, q_pos, key_docs, m, l, acc, ctx, res, d2d_src, d2d_dst, y_src, y_dst, fin,
    q_sem, doc_sem, own_sem, w_sem, recv_sem, zsend_sem, xsend_sem,
    d2d_send, d2d_recv, y_send, y_recv,
):
    s = lax.axis_index("seq")
    t = lax.axis_index("tp")
    tokens = q_hbm.shape[0]
    heads_kv = k_hbm.shape[1] // HD
    pieces = 4 * heads_kv
    half = tokens // 2
    late = pieces // 4
    chips = n_tp // 2
    rows = tokens // n_tp
    width = out_ref.shape[1] // CHUNKS
    odd = s % 2
    partner = s + 1 - 2 * odd
    core = t % 2
    chip = t // 2
    sibling = t + 1 - 2 * core
    tile = math.gcd(GROUP * tokens, 256)

    def q_copy():
        return pltpu.make_async_copy(q_hbm, q_all, q_sem)

    def doc_copy():
        return pltpu.make_async_copy(doc_hbm, docs, doc_sem)

    def own_copy(c):
        src = k_hbm if c % 4 < 2 else v_hbm
        return pltpu.make_async_copy(
            src.at[pl.ds((c % 2) * half, half), pl.ds((c // 4) * HD, HD)],
            kv.at[0, c], own_sem.at[c],
        )

    def w_copy(j):
        cols = pl.ds(pl.multiple_of(j * width, width), width)
        return pltpu.make_async_copy(w_hbm.at[:, cols], w.at[:, cols], w_sem.at[j])

    for c in range(pieces):
        own_copy(c).start()
    q_copy().start()
    doc_copy().start()

    barrier = pltpu.get_barrier_semaphore()

    def greet(seq_index, tp_index):
        pl.semaphore_signal(
            barrier, inc=1, device_id=(seq_index, tp_index), device_id_type=MESH
        )

    greet(partner, t)
    greet(s, sibling)
    for step in range(1, chips):
        greet(s, ((chip + step) % chips) * 2 + core)

    @pl.when(s >= 2)
    def _():
        greet(s - 2, t)

    @pl.when(s + 2 < n_seq)
    def _():
        greet(s + 2, t)

    for j in range(CHUNKS):
        w_copy(j).start()

    along = (s >= 2).astype(jnp.int32) + (s + 2 < n_seq).astype(jnp.int32)
    pl.semaphore_wait(barrier, chips + 1 + along)

    def z_copy(d, c):
        return pltpu.make_async_remote_copy(
            src_ref=kv.at[d, c], dst_ref=kv.at[d + 2, c],
            send_sem=zsend_sem.at[d, c], recv_sem=recv_sem.at[d + 2, c],
            device_id=(s + 2, t), device_id_type=MESH,
        )

    def x_copy(d, to, c):
        return pltpu.make_async_remote_copy(
            src_ref=kv.at[d, c], dst_ref=kv.at[to, c],
            send_sem=xsend_sem.at[d, c], recv_sem=recv_sem.at[to, c],
            device_id=(partner, t), device_id_type=MESH,
        )

    def arrival(d, c):
        return pltpu.make_async_remote_copy(
            src_ref=kv.at[d, c], dst_ref=kv.at[d, c],
            send_sem=xsend_sem.at[d, c], recv_sem=recv_sem.at[d, c],
            device_id=(partner, t), device_id_type=MESH,
        )

    def for_sends(d, act):
        if d % 2 == 1:
            if d + 2 <= reach:
                @pl.when((s >= d) & (odd == 0) & (s + 2 < n_seq))
                def _():
                    act(lambda c: z_copy(d, c), range(pieces - late, pieces))
            return
        if d + 2 <= reach:
            @pl.when((s >= d) & (s + 2 < n_seq))
            def _():
                act(lambda c: z_copy(d, c), range(pieces))
        if d + 1 <= reach:
            @pl.when((s >= d) & (odd == 0))
            def _():
                act(lambda c: x_copy(d, d + 1, c), range(pieces))
        if d >= 2:
            @pl.when((s >= d) & (odd == 1))
            def _():
                act(lambda c: x_copy(d, d - 1, c), range(pieces if d == 2 else pieces - late))

    def take(d, c):
        arrival(d, c).wait_recv()

        def pass_on(copy, which):
            @pl.when((c >= which.start) & (c < which.stop))
            def _():
                copy(c).start()

        for_sends(d, pass_on)

    for c in range(pieces):
        own_copy(c).wait()
        for_sends(0, lambda copy, which, c=c: copy(c).start())

    q_copy().wait()
    for h in range(heads_kv * GROUP):
        q[h // GROUP, pl.ds((h % GROUP) * tokens, tokens), :] = q_all[:, h * HD:(h + 1) * HD]

    doc_copy().wait()
    lanes = 128
    span = (tokens + lanes - math.gcd(tokens, lanes) + lanes - 1) // lanes
    key_of = lax.broadcasted_iota(jnp.int32, (tokens, span * lanes), 0)
    lane_of = lax.broadcasted_iota(jnp.int32, (tokens, span * lanes), 1)

    def docs_down(block):
        first = block * tokens
        top_row, shift = first // lanes, first % lanes
        ids = jnp.concatenate(
            [
                docs[pl.ds(jnp.minimum(top_row + i, docs.shape[0] - 1), 1), :]
                for i in range(span)
            ],
            axis=1,
        ).astype(jnp.float32)
        return jnp.sum(jnp.where(lane_of == key_of + shift, ids, 0.0), axis=1, keepdims=True)

    row_of = lax.broadcasted_iota(jnp.int32, (tokens, tokens), 0)
    col_of = lax.broadcasted_iota(jnp.int32, (tokens, tokens), 1)
    own_row = jnp.sum(
        jnp.where(row_of == col_of, docs_down(s), 0.0), axis=0, keepdims=True
    )
    q_doc[...] = jnp.concatenate([own_row] * GROUP, axis=1)
    q_pos[...] = jnp.concatenate([col_of[:1]] * GROUP, axis=1)
    tiles = [pl.ds(i * tile, tile) for i in range(GROUP * tokens // tile)]

    def attend(d, g):
        key_doc = key_docs[...]
        keys = kv[d, pl.ds(4 * g, 2)].reshape(tokens, HD)
        probs = []
        for cols in tiles:
            scores = lax.dot_general(
                keys, q[g, cols, :], (((1,), (1,)), ((), ())),
                preferred_element_type=jnp.float32,
            )
            allowed = key_doc == q_doc[:, cols]
            if d == 0:
                key_pos = lax.broadcasted_iota(jnp.int32, (tokens, tile), 0)
                allowed = allowed & (key_pos <= q_pos[:, cols])
            scores = jnp.where(allowed, scores * SCALE, MASKED)
            top = jnp.max(scores, axis=0, keepdims=True)
            if d == 0:
                p = jnp.exp2(scores - top)
                l[g, :, cols] = jnp.sum(p, axis=0, keepdims=True)
                m[g, :, cols] = top
                rescale = None
            else:
                old_m = m[g, :, cols]
                new_m = jnp.maximum(old_m, top)
                p = jnp.exp2(scores - new_m)
                rescale = jnp.exp2(old_m - new_m)
                l[g, :, cols] = l[g, :, cols] * rescale + jnp.sum(p, axis=0, keepdims=True)
                m[g, :, cols] = new_m
            probs.append((p.astype(jnp.bfloat16), rescale))
        if d > 0:
            take(d, 4 * g + 2)
            take(d, 4 * g + 3)
        values = kv[d, pl.ds(4 * g + 2, 2)].reshape(tokens, HD)
        for cols, (p, rescale) in zip(tiles, probs):
            added = lax.dot_general(
                values, p, (((0,), (0,)), ((), ())),
                preferred_element_type=jnp.float32,
            )
            if d == 0:
                acc[g, :, cols] = added
            else:
                acc[g, :, cols] = acc[g, :, cols] * rescale + added

    order = [0]
    for d in range(2, reach + 1, 2):
        order += [d, d - 1]
    def visit(d, g):
        if d > 0:
            take(d, 4 * g)
            take(d, 4 * g + 1)
        attend(d, g)

    for d in order[:-1]:
        @pl.when(s >= d)
        def _(d=d):
            key_docs[...] = docs_down(s - d)

            @pl.loop(0, heads_kv)
            def _(g):
                visit(d, g)

    last = order[-1]

    @pl.when(s >= last)
    def _():
        key_docs[...] = docs_down(s - last)

    for g in range(heads_kv):
        @pl.when(s >= last)
        def _(g=g):
            visit(last, g)

        mixed = jnp.transpose(acc[g] / l[g]).astype(jnp.bfloat16)
        for i in range(GROUP):
            h = g * GROUP + i
            ctx[:, h * HD:(h + 1) * HD] = mixed[i * tokens:(i + 1) * tokens, :]

    def d2d_copy(j):
        return pltpu.make_async_remote_copy(
            src_ref=d2d_src.at[j], dst_ref=d2d_dst.at[j],
            send_sem=d2d_send.at[j], recv_sem=d2d_recv.at[j],
            device_id=(s, sibling), device_id_type=MESH,
        )

    def y_copy(j, step):
        return pltpu.make_async_remote_copy(
            src_ref=y_src.at[j, step - 1], dst_ref=y_dst.at[j, step - 1],
            send_sem=y_send.at[j, step - 1], recv_sem=y_recv.at[j, step - 1],
            device_id=(s, ((chip + step) % chips) * 2 + core), device_id_type=MESH,
        )

    def rows_of(j, owner):
        return res[j % 2, pl.ds(pl.multiple_of(owner * rows, 8), rows), :]

    def project(j):
        w_copy(j).wait()
        cols = pl.ds(pl.multiple_of(j * width, width), width)
        res[j % 2] = jnp.dot(ctx[...], w[:, cols], preferred_element_type=jnp.float32)
        for y in range(chips):
            d2d_src[j, y] = rows_of(j, y * 2 + 1 - core).astype(jnp.bfloat16)
        d2d_copy(j).start()

    def pair_up(j):
        d2d_copy(j).wait_recv()
        for step in range(1, chips):
            other = (chip + step) % chips
            pair = rows_of(j, other * 2 + core) + d2d_dst[j, other].astype(jnp.float32)
            y_src[j, step - 1] = pair.astype(jnp.bfloat16)
            y_copy(j, step).start()
        fin[j] = rows_of(j, t) + d2d_dst[j, chip].astype(jnp.float32)

    project(0)

    @pl.loop(1, CHUNKS)
    def _(j):
        project(j)
        pair_up(j - 1)

    pair_up(CHUNKS - 1)

    @pl.loop(0, CHUNKS)
    def _(j):
        total = fin[j]
        for step in range(1, chips):
            y_copy(j, step).wait_recv()
            total = total + y_dst[j, step - 1].astype(jnp.float32)
        cols = pl.ds(pl.multiple_of(j * width, width), width)
        out_ref[:, cols] = total.astype(out_ref.dtype)

    for d in range(reach + 1):
        def drain(copy, which):
            for c in which:
                copy(c).wait_send()
        for_sends(d, drain)

    @pl.loop(0, CHUNKS)
    def _(j):
        d2d_copy(j).wait_send()
        for step in range(1, chips):
            y_copy(j, step).wait_send()


def solution(mesh):
    n_seq, n_tp = mesh.shape["seq"], mesh.shape["tp"]
    reach = min(12, n_seq // 2)
    chips = n_tp // 2

    def per_device(query_rows, key_rows, value_rows, document_ids, output_weight):
        tokens, q_width = query_rows.shape
        heads_kv = key_rows.shape[1] // HD
        depth, model = output_weight.shape
        rows, width = tokens // n_tp, model // CHUNKS
        bf16, f32 = jnp.bfloat16, jnp.float32
        dma = pltpu.SemaphoreType.DMA
        docs = document_ids.reshape(-1, 128)
        in_hbm = pl.BlockSpec(memory_space=pltpu.HBM)
        in_vmem = pl.BlockSpec(memory_space=pltpu.VMEM)
        return pl.pallas_call(
            functools.partial(kernel, n_seq, n_tp, reach),
            out_shape=pltpu.VMEM((rows, model), bf16),
            in_specs=[in_hbm] * 5,
            out_specs=in_vmem,
            scratch_shapes=[
                pltpu.VMEM((tokens, q_width), bf16),
                pltpu.VMEM((heads_kv, GROUP * tokens, HD), bf16),
                pltpu.VMEM((reach + 1, 4 * heads_kv, tokens // 2, HD), bf16),
                pltpu.VMEM((depth, model), bf16),
                pltpu.VMEM(docs.shape, jnp.int32),
                pltpu.VMEM((1, GROUP * tokens), f32),
                pltpu.VMEM((1, GROUP * tokens), jnp.int32),
                pltpu.VMEM((tokens, 1), f32),
                pltpu.VMEM((heads_kv, 1, GROUP * tokens), f32),
                pltpu.VMEM((heads_kv, 1, GROUP * tokens), f32),
                pltpu.VMEM((heads_kv, HD, GROUP * tokens), f32),
                pltpu.VMEM((tokens, q_width), bf16),
                pltpu.VMEM((2, tokens, width), f32),
                pltpu.VMEM((CHUNKS, chips, rows, width), bf16),
                pltpu.VMEM((CHUNKS, chips, rows, width), bf16),
                pltpu.VMEM((CHUNKS, chips - 1, rows, width), bf16),
                pltpu.VMEM((CHUNKS, chips - 1, rows, width), bf16),
                pltpu.VMEM((CHUNKS, rows, width), f32),
                dma, dma, dma((4 * heads_kv,)), dma((CHUNKS,)),
                dma((reach + 1, 4 * heads_kv)),
                dma((reach + 1, 4 * heads_kv)),
                dma((reach + 1, 4 * heads_kv)),
                dma((CHUNKS,)), dma((CHUNKS,)),
                dma((CHUNKS, chips - 1)), dma((CHUNKS, chips - 1)),
            ],
            compiler_params=pltpu.CompilerParams(
                collective_id=0, has_side_effects=True, vmem_limit_bytes=60 * 1024 * 1024
            ),
        )(query_rows, key_rows, value_rows, docs, output_weight)

    in_specs = (P("seq", "tp"), P("seq", "tp"), P("seq", "tp"), P(), P("tp", None))
    return jax.shard_map(
        per_device, mesh=mesh, in_specs=in_specs, out_specs=P(("seq", "tp"), None),
        check_vma=False,
    )
```

```python
import functools
import math

import jax
import jax.numpy as jnp
from jax import lax
from jax.experimental import pallas as pl
from jax.experimental.pallas import tpu as pltpu
from jax.sharding import PartitionSpec as P

HEADS = 32
KV = 8
HD = 128
GROUP = HEADS // KV
MESH = pl.DeviceIdType.MESH
LOG2E = 1.4426950408889634
SCALE = LOG2E / HD**0.5
MASKED = -1e30
CHUNKS = 8


def kernel(
    n_seq, n_tp, reach,
    q_hbm, k_hbm, v_hbm, doc_hbm, w_hbm, out_ref,
    q_all, q, kv, w, docs, q_doc, q_pos, key_docs, m, l, acc, ctx, res, d2d_src, d2d_dst, y_src, y_dst, fin,
    q_sem, doc_sem, own_sem, w_sem, recv_sem, zsend_sem, xsend_sem,
    d2d_send, d2d_recv, y_send, y_recv,
):
    s = lax.axis_index("seq")
    t = lax.axis_index("tp")
    tokens = q_hbm.shape[0]
    heads_kv = k_hbm.shape[1] // HD
    pieces = 4 * heads_kv
    half = tokens // 2
    late = pieces // 4
    chips = n_tp // 2
    rows = tokens // n_tp
    width = out_ref.shape[1] // CHUNKS
    odd = s % 2
    partner = s + 1 - 2 * odd
    core = t % 2
    chip = t // 2
    sibling = t + 1 - 2 * core
    tile = math.gcd(GROUP * tokens, 256)

    def q_copy():
        return pltpu.make_async_copy(q_hbm, q_all, q_sem)

    def doc_copy():
        return pltpu.make_async_copy(doc_hbm, docs, doc_sem)

    def own_copy(c):
        src = k_hbm if c % 4 < 2 else v_hbm
        return pltpu.make_async_copy(
            src.at[pl.ds((c % 2) * half, half), pl.ds((c // 4) * HD, HD)],
            kv.at[0, c], own_sem.at[c],
        )

    def w_copy(j):
        cols = pl.ds(pl.multiple_of(j * width, width), width)
        return pltpu.make_async_copy(w_hbm.at[:, cols], w.at[:, cols], w_sem.at[j])

    for c in range(pieces):
        own_copy(c).start()
    q_copy().start()
    doc_copy().start()

    barrier = pltpu.get_barrier_semaphore()

    def greet(seq_index, tp_index):
        pl.semaphore_signal(
            barrier, inc=1, device_id=(seq_index, tp_index), device_id_type=MESH
        )

    greet(partner, t)
    greet(s, sibling)
    for step in range(1, chips):
        greet(s, ((chip + step) % chips) * 2 + core)

    @pl.when(s >= 2)
    def _():
        greet(s - 2, t)

    @pl.when(s + 2 < n_seq)
    def _():
        greet(s + 2, t)

    for j in range(CHUNKS):
        w_copy(j).start()

    along = (s >= 2).astype(jnp.int32) + (s + 2 < n_seq).astype(jnp.int32)
    pl.semaphore_wait(barrier, chips + 1 + along)

    def z_copy(d, c):
        return pltpu.make_async_remote_copy(
            src_ref=kv.at[d, c], dst_ref=kv.at[d + 2, c],
            send_sem=zsend_sem.at[d, c], recv_sem=recv_sem.at[d + 2, c],
            device_id=(s + 2, t), device_id_type=MESH,
        )

    def x_copy(d, to, c):
        return pltpu.make_async_remote_copy(
            src_ref=kv.at[d, c], dst_ref=kv.at[to, c],
            send_sem=xsend_sem.at[d, c], recv_sem=recv_sem.at[to, c],
            device_id=(partner, t), device_id_type=MESH,
        )

    def arrival(d, c):
        return pltpu.make_async_remote_copy(
            src_ref=kv.at[d, c], dst_ref=kv.at[d, c],
            send_sem=xsend_sem.at[d, c], recv_sem=recv_sem.at[d, c],
            device_id=(partner, t), device_id_type=MESH,
        )

    def for_sends(d, act):
        if d % 2 == 1:
            if d + 2 <= reach:
                @pl.when((s >= d) & (odd == 0) & (s + 2 < n_seq))
                def _():
                    act(lambda c: z_copy(d, c), range(pieces - late, pieces))
            return
        if d + 2 <= reach:
            @pl.when((s >= d) & (s + 2 < n_seq))
            def _():
                act(lambda c: z_copy(d, c), range(pieces))
        if d + 1 <= reach:
            @pl.when((s >= d) & (odd == 0))
            def _():
                act(lambda c: x_copy(d, d + 1, c), range(pieces))
        if d >= 2:
            @pl.when((s >= d) & (odd == 1))
            def _():
                act(lambda c: x_copy(d, d - 1, c), range(pieces if d == 2 else pieces - late))

    def take(d, c):
        arrival(d, c).wait_recv()

        def pass_on(copy, which):
            @pl.when((c >= which.start) & (c < which.stop))
            def _():
                copy(c).start()

        for_sends(d, pass_on)

    for c in range(pieces):
        own_copy(c).wait()
        for_sends(0, lambda copy, which, c=c: copy(c).start())

    q_copy().wait()
    for h in range(heads_kv * GROUP):
        q[h // GROUP, pl.ds((h % GROUP) * tokens, tokens), :] = q_all[:, h * HD:(h + 1) * HD]

    doc_copy().wait()
    lanes = 128
    span = (tokens + lanes - math.gcd(tokens, lanes) + lanes - 1) // lanes
    key_of = lax.broadcasted_iota(jnp.int32, (tokens, span * lanes), 0)
    lane_of = lax.broadcasted_iota(jnp.int32, (tokens, span * lanes), 1)

    def docs_down(block):
        first = block * tokens
        top_row, shift = first // lanes, first % lanes
        ids = jnp.concatenate(
            [
                docs[pl.ds(jnp.minimum(top_row + i, docs.shape[0] - 1), 1), :]
                for i in range(span)
            ],
            axis=1,
        ).astype(jnp.float32)
        return jnp.sum(jnp.where(lane_of == key_of + shift, ids, 0.0), axis=1, keepdims=True)

    row_of = lax.broadcasted_iota(jnp.int32, (tokens, tokens), 0)
    col_of = lax.broadcasted_iota(jnp.int32, (tokens, tokens), 1)
    own_row = jnp.sum(
        jnp.where(row_of == col_of, docs_down(s), 0.0), axis=0, keepdims=True
    )
    q_doc[...] = jnp.concatenate([own_row] * GROUP, axis=1)
    q_pos[...] = jnp.concatenate([col_of[:1]] * GROUP, axis=1)
    tiles = [pl.ds(i * tile, tile) for i in range(GROUP * tokens // tile)]

    def attend(d, g):
        key_doc = key_docs[...]
        keys = kv[d, pl.ds(4 * g, 2)].reshape(tokens, HD)
        probs = []
        for cols in tiles:
            scores = lax.dot_general(
                keys, q[g, cols, :], (((1,), (1,)), ((), ())),
                preferred_element_type=jnp.float32,
            )
            allowed = key_doc == q_doc[:, cols]
            if d == 0:
                key_pos = lax.broadcasted_iota(jnp.int32, (tokens, tile), 0)
                allowed = allowed & (key_pos <= q_pos[:, cols])
            scores = jnp.where(allowed, scores * SCALE, MASKED)
            top = jnp.max(scores, axis=0, keepdims=True)
            if d == 0:
                p = jnp.exp2(scores - top)
                l[g, :, cols] = jnp.sum(p, axis=0, keepdims=True)
                m[g, :, cols] = top
                rescale = None
            else:
                old_m = m[g, :, cols]
                new_m = jnp.maximum(old_m, top)
                p = jnp.exp2(scores - new_m)
                rescale = jnp.exp2(old_m - new_m)
                l[g, :, cols] = l[g, :, cols] * rescale + jnp.sum(p, axis=0, keepdims=True)
                m[g, :, cols] = new_m
            probs.append((p.astype(jnp.bfloat16), rescale))
        if d > 0:
            take(d, 4 * g + 2)
            take(d, 4 * g + 3)
        values = kv[d, pl.ds(4 * g + 2, 2)].reshape(tokens, HD)
        for cols, (p, rescale) in zip(tiles, probs):
            added = lax.dot_general(
                values, p, (((0,), (0,)), ((), ())),
                preferred_element_type=jnp.float32,
            )
            if d == 0:
                acc[g, :, cols] = added
            else:
                acc[g, :, cols] = acc[g, :, cols] * rescale + added

    order = [0]
    for d in range(2, reach + 1, 2):
        order += [d, d - 1]
    def visit(d, g):
        if d > 0:
            take(d, 4 * g)
            take(d, 4 * g + 1)
        attend(d, g)

    for d in order[:-1]:
        @pl.when(s >= d)
        def _(d=d):
            key_docs[...] = docs_down(s - d)

            @pl.loop(0, heads_kv)
            def _(g):
                visit(d, g)

    last = order[-1]

    @pl.when(s >= last)
    def _():
        key_docs[...] = docs_down(s - last)

    for g in range(heads_kv):
        @pl.when(s >= last)
        def _(g=g):
            visit(last, g)

        mixed = jnp.transpose(acc[g] / l[g]).astype(jnp.bfloat16)
        for i in range(GROUP):
            h = g * GROUP + i
            ctx[:, h * HD:(h + 1) * HD] = mixed[i * tokens:(i + 1) * tokens, :]

    def d2d_copy(j):
        return pltpu.make_async_remote_copy(
            src_ref=d2d_src.at[j], dst_ref=d2d_dst.at[j],
            send_sem=d2d_send.at[j], recv_sem=d2d_recv.at[j],
            device_id=(s, sibling), device_id_type=MESH,
        )

    def y_copy(j, step):
        return pltpu.make_async_remote_copy(
            src_ref=y_src.at[j, step - 1], dst_ref=y_dst.at[j, step - 1],
            send_sem=y_send.at[j, step - 1], recv_sem=y_recv.at[j, step - 1],
            device_id=(s, ((chip + step) % chips) * 2 + core), device_id_type=MESH,
        )

    def rows_of(j, owner):
        return res[j % 2, pl.ds(pl.multiple_of(owner * rows, 8), rows), :]

    def project(j):
        w_copy(j).wait()
        cols = pl.ds(pl.multiple_of(j * width, width), width)
        res[j % 2] = jnp.dot(ctx[...], w[:, cols], preferred_element_type=jnp.float32)
        for y in range(chips):
            d2d_src[j, y] = rows_of(j, y * 2 + 1 - core).astype(jnp.bfloat16)
        d2d_copy(j).start()

    def pair_up(j):
        d2d_copy(j).wait_recv()
        for step in range(1, chips):
            other = (chip + step) % chips
            pair = rows_of(j, other * 2 + core) + d2d_dst[j, other].astype(jnp.float32)
            y_src[j, step - 1] = pair.astype(jnp.bfloat16)
            y_copy(j, step).start()
        fin[j] = rows_of(j, t) + d2d_dst[j, chip].astype(jnp.float32)

    project(0)

    @pl.loop(1, CHUNKS)
    def _(j):
        project(j)
        pair_up(j - 1)

    pair_up(CHUNKS - 1)

    @pl.loop(0, CHUNKS)
    def _(j):
        total = fin[j]
        for step in range(1, chips):
            y_copy(j, step).wait_recv()
            total = total + y_dst[j, step - 1].astype(jnp.float32)
        cols = pl.ds(pl.multiple_of(j * width, width), width)
        out_ref[:, cols] = total.astype(out_ref.dtype)

    for d in range(reach + 1):
        def drain(copy, which):
            for c in which:
                copy(c).wait_send()
        for_sends(d, drain)

    @pl.loop(0, CHUNKS)
    def _(j):
        d2d_copy(j).wait_send()
        for step in range(1, chips):
            y_copy(j, step).wait_send()


def solution(mesh):
    n_seq, n_tp = mesh.shape["seq"], mesh.shape["tp"]
    reach = min(12, n_seq // 2)
    chips = n_tp // 2

    def per_device(query_rows, key_rows, value_rows, document_ids, output_weight):
        tokens, q_width = query_rows.shape
        heads_kv = key_rows.shape[1] // HD
        depth, model = output_weight.shape
        rows, width = tokens // n_tp, model // CHUNKS
        bf16, f32 = jnp.bfloat16, jnp.float32
        dma = pltpu.SemaphoreType.DMA
        docs = document_ids.reshape(-1, 128)
        in_hbm = pl.BlockSpec(memory_space=pltpu.HBM)
        in_vmem = pl.BlockSpec(memory_space=pltpu.VMEM)
        return pl.pallas_call(
            functools.partial(kernel, n_seq, n_tp, reach),
            out_shape=pltpu.VMEM((rows, model), bf16),
            in_specs=[in_hbm] * 5,
            out_specs=in_vmem,
            scratch_shapes=[
                pltpu.VMEM((tokens, q_width), bf16),
                pltpu.VMEM((heads_kv, GROUP * tokens, HD), bf16),
                pltpu.VMEM((reach + 1, 4 * heads_kv, tokens // 2, HD), bf16),
                pltpu.VMEM((depth, model), bf16),
                pltpu.VMEM(docs.shape, jnp.int32),
                pltpu.VMEM((1, GROUP * tokens), f32),
                pltpu.VMEM((1, GROUP * tokens), jnp.int32),
                pltpu.VMEM((tokens, 1), f32),
                pltpu.VMEM((heads_kv, 1, GROUP * tokens), f32),
                pltpu.VMEM((heads_kv, 1, GROUP * tokens), f32),
                pltpu.VMEM((heads_kv, HD, GROUP * tokens), f32),
                pltpu.VMEM((tokens, q_width), bf16),
                pltpu.VMEM((2, tokens, width), f32),
                pltpu.VMEM((CHUNKS, chips, rows, width), bf16),
                pltpu.VMEM((CHUNKS, chips, rows, width), bf16),
                pltpu.VMEM((CHUNKS, chips - 1, rows, width), bf16),
                pltpu.VMEM((CHUNKS, chips - 1, rows, width), bf16),
                pltpu.VMEM((CHUNKS, rows, width), f32),
                dma, dma, dma((4 * heads_kv,)), dma((CHUNKS,)),
                dma((reach + 1, 4 * heads_kv)),
                dma((reach + 1, 4 * heads_kv)),
                dma((reach + 1, 4 * heads_kv)),
                dma((CHUNKS,)), dma((CHUNKS,)),
                dma((CHUNKS, chips - 1)), dma((CHUNKS, chips - 1)),
            ],
            compiler_params=pltpu.CompilerParams(
                collective_id=0, has_side_effects=True, vmem_limit_bytes=60 * 1024 * 1024
            ),
        )(query_rows, key_rows, value_rows, docs, output_weight)

    in_specs = (P("seq", "tp"), P("seq", "tp"), P("seq", "tp"), P(), P("tp", None))
    return jax.shard_map(
        per_device, mesh=mesh, in_specs=in_specs, out_specs=P(("seq", "tp"), None),
        check_vma=False,
    )
```
